32 devices in a mesh: shard: 8 (over z, y), width: 4 (over x, core).
Axes of the slice: x: 2, y: 2, z: 4, core: 2. Of those that a mesh axis runs over, the one named last changes fastest.
Arguments:
- one_query: float32 [3584, 4096], P('shard', 'width'), may hold values from -0.125 to 0.125
- other_query: float32 [3584, 4096], P('shard', 'width'), may hold values from -0.09375 to 0.09375
- one_key: float32 [3584, 2048], P('shard', 'width'), may hold values from -0.125 to 0.125
- other_key: float32 [3584, 2048], P('shard', 'width'), may hold values from -0.09375 to 0.09375
- one_value: float32 [3584, 2048], P('shard', 'width'), may hold values from -0.125 to 0.125
- other_value: float32 [3584, 2048], P('shard', 'width'), may hold values from -0.09375 to 0.09375
- mix_share: float32 [3584], P('shard'), may hold values from 0.2 to 0.8
- norm_gain: float32 [3584], P('shard'), may hold values from 0.25 to 1.75
Outputs:
- final_query: bfloat16 [3584, 4096], P(None, 'width')
- final_key: bfloat16 [3584, 2048], P(None, 'width')
- final_value: bfloat16 [3584, 2048], P(None, 'width')
- scale_query: float32 [4096], P('width')
- scale_key: float32 [2048], P('width')
- scale_value: float32 [2048], P('width')
The draws below stay inside these ranges and needn't reach their ends.
All inputs are finite; a program needn't handle non-finite values.
Results may differ from the reference program's by a relative error of at most 0.001.
Values may be sent and summed in bfloat16 or wider, within the bound.
A program may use at most 128 MiB of HBM per device.

```python
import jax
import jax.numpy as jnp
from jax import lax

D_MODEL = 3584
Q_DIM = 4096
KV_DIM = 2048


def raised(array, own_key, source, target, blocks, factor):
    def block_of(axis_at):
        return (jnp.arange(array.shape[axis_at]) // (array.shape[axis_at] // blocks)).reshape((-1,) + (1,) * (array.ndim - 1 - axis_at))

    first = jax.random.permutation(own_key, blocks)[block_of(target)]
    second = (block_of(target) + blocks // 2) % blocks
    return jnp.where((block_of(source) == first) | (block_of(source) == second), factor * array, array)


def shard_levels(own_key, dims, cuts, low, top_value):
    loudness, own = 1.0, jax.random.fold_in(own_key, 6)
    for position, parts in cuts:
        draws = jnp.exp(jax.random.uniform(jax.random.fold_in(own, position), (parts,), jnp.float32, low / len(cuts), top_value / len(cuts)))
        loudness = loudness * jnp.repeat(draws, dims[position] // parts).reshape([-1 if axis == position else 1 for axis in range(len(dims))])
    return loudness


def normal_values(rng, shape, width, most, pieces=(), dtype=jnp.bfloat16):
    factor_of = shard_levels(rng, shape, pieces, -0.22, 0.18) if pieces else 1.0
    result = jax.random.normal(rng, shape, jnp.float32) * width * factor_of
    return jnp.minimum(jnp.maximum(result, -most), most).astype(dtype)


def bell_draw_with(own_key, extent, scale, most, cuts, heavy, kind=jnp.bfloat16):
    values = scale * jax.random.normal(own_key, extent, jnp.float32)
    if cuts:
        values = values * shard_levels(own_key, extent, cuts, -0.22, 0.18)
    return jnp.clip(raised(values, jax.random.fold_in(own_key, 3), *heavy), -most, most).astype(kind)


def setup_inputs(seed: int = 0) -> dict:
    key_list = jax.random.split(jax.random.key(seed), 9)
    one_query = bell_draw_with(key_list[0], (D_MODEL, Q_DIM), D_MODEL ** -0.5, 0.125, ((0, 8), (1, 4)), (0, 1, 8, 2.0), jnp.float32)
    other_query = normal_values(key_list[1], (D_MODEL, Q_DIM), D_MODEL ** -0.5, 0.09375, ((0, 8), (1, 4)), jnp.float32)
    one_key = bell_draw_with(key_list[2], (D_MODEL, KV_DIM), D_MODEL ** -0.5, 0.125, ((0, 8), (1, 4)), (0, 1, 8, 2.0), jnp.float32)
    other_key = normal_values(key_list[3], (D_MODEL, KV_DIM), D_MODEL ** -0.5, 0.09375, ((0, 8), (1, 4)), jnp.float32)
    one_value = bell_draw_with(key_list[4], (D_MODEL, KV_DIM), D_MODEL ** -0.5, 0.125, ((0, 8), (1, 4)), (0, 1, 8, 2.0), jnp.float32)
    other_value = normal_values(key_list[5], (D_MODEL, KV_DIM), D_MODEL ** -0.5, 0.09375, ((0, 8), (1, 4)), jnp.float32)
    mix_share = jnp.clip(0.2 + 0.6 * jax.random.uniform(key_list[6], (D_MODEL,), jnp.float32) ** shard_levels(key_list[6], (D_MODEL,), ((0, 8),), -0.2, 0.2), 0.2, 0.8)
    norm_gain = jnp.clip(1.0 + 0.15 * jax.random.normal(key_list[7], (D_MODEL,), jnp.float32), 0.25, 1.75)
    return {"one_query": one_query, "other_query": other_query, "one_key": one_key, "other_key": other_key, "one_value": one_value, "other_value": other_value, "mix_share": mix_share, "norm_gain": norm_gain}


def reference(one_query, other_query, one_key, other_key, one_value, other_value, mix_share, norm_gain):
    result_query = mix_share[:, None] * one_query + (1.0 - mix_share[:, None]) * other_query
    result_key = mix_share[:, None] * one_key + (1.0 - mix_share[:, None]) * other_key
    result_value = mix_share[:, None] * one_value + (1.0 - mix_share[:, None]) * other_value
    result_gained_query = result_query * norm_gain[:, None]
    result_gained_key = result_key * norm_gain[:, None]
    result_gained_value = result_value * norm_gain[:, None]
    scale_query = jnp.sqrt(lax.optimization_barrier(jnp.sum(result_gained_query * result_gained_query, axis=0)))
    final_query = (result_gained_query / scale_query).astype(jnp.bfloat16)
    scale_key = jnp.sqrt(lax.optimization_barrier(jnp.sum(result_gained_key * result_gained_key, axis=0)))
    final_key = (result_gained_key / scale_key).astype(jnp.bfloat16)
    scale_value = jnp.sqrt(lax.optimization_barrier(jnp.sum(result_gained_value * result_gained_value, axis=0)))
    final_value = (result_gained_value / scale_value).astype(jnp.bfloat16)
    return (final_query, final_key, final_value, scale_query, scale_key, scale_value)
```

```python
import functools

import jax
import jax.numpy as jnp
from jax import lax
from jax.experimental import pallas as pl
from jax.experimental.pallas import tpu as pltpu
from jax.sharding import PartitionSpec as P

MESH = pl.DeviceIdType.MESH
ROWS = 16


def plain(one_query, other_query, one_key, other_key, one_value, other_value, mix_share, norm_gain):
    result_query = mix_share[:, None] * one_query + (1.0 - mix_share[:, None]) * other_query
    result_key = mix_share[:, None] * one_key + (1.0 - mix_share[:, None]) * other_key
    result_value = mix_share[:, None] * one_value + (1.0 - mix_share[:, None]) * other_value
    result_gained_query = result_query * norm_gain[:, None]
    result_gained_key = result_key * norm_gain[:, None]
    result_gained_value = result_value * norm_gain[:, None]
    total_query, total_key, total_value = lax.psum(
        (
            jnp.sum(result_gained_query * result_gained_query, axis=0),
            jnp.sum(result_gained_key * result_gained_key, axis=0),
            jnp.sum(result_gained_value * result_gained_value, axis=0),
        ),
        "shard",
    )
    scale_query = jnp.sqrt(total_query)
    scale_key = jnp.sqrt(total_key)
    scale_value = jnp.sqrt(total_value)
    narrow_query, narrow_key, narrow_value = (
        (result_gained_query / scale_query).astype(jnp.bfloat16),
        (result_gained_key / scale_key).astype(jnp.bfloat16),
        (result_gained_value / scale_value).astype(jnp.bfloat16),
    )
    final_query, final_key, final_value = (
        lax.all_gather(narrow_query, "shard", axis=0, tiled=True),
        lax.all_gather(narrow_key, "shard", axis=0, tiled=True),
        lax.all_gather(narrow_value, "shard", axis=0, tiled=True),
    )
    return (final_query, final_key, final_value, scale_query, scale_key, scale_value)


def cuts(blocks, parts):
    edges = [blocks * part // parts for part in range(parts + 1)]
    return [(low * ROWS, (high - low) * ROWS) for low, high in zip(edges, edges[1:])]


def plan(rows, line):
    blocks = rows // ROWS
    far = max(1, round(blocks / (2 * (line - 1)))) if line > 1 else 0
    pieces = cuts(blocks - far, 5)
    near = len(pieces)
    if far:
        pieces.append(((blocks - far) * ROWS, far * ROWS))
    return pieces, near


def gather_kernel(n, widths, share_ref, gain_ref, *refs):
    ins, (buf, scale_ref, first, second, sums, in_sem, sum_send, sum_recv, send_sem, recv_sem) = refs[:6], refs[6:]
    rows = first.shape[0]
    total = sum(widths)
    line = n // 2
    me = lax.axis_index("shard")
    z, y = me // 2, me % 2
    other = z * 2 + 1 - y
    pieces, near = plan(rows, line)
    starts = [sum(widths[:i]) for i in range(len(widths))]

    loads = []
    parts = cuts(rows // ROWS, 4)
    for p, (low, size) in enumerate(parts):
        group = []
        for i, ref in enumerate(ins):
            dest = (first, second)[i % 2].at[pl.ds(low, size), pl.ds(starts[i // 2], widths[i // 2])]
            copy = pltpu.make_async_copy(ref.at[pl.ds(low, size), :], dest, in_sem.at[p, i])
            copy.start()
            group.append(copy)
        loads.append(group)

    barrier = pltpu.get_barrier_semaphore()
    for step in range(1, n):
        pl.semaphore_signal(barrier, inc=1, device_id={"shard": lax.rem(me + step, n)}, device_id_type=MESH)

    def mixed(block, acc):
        at = pl.ds(pl.multiple_of(block * ROWS, ROWS), ROWS)
        share, gain = share_ref[at, :], gain_ref[at, :]
        left, right = share * gain, (1.0 - share) * gain
        out = []
        for i in range(len(acc)):
            cols = pl.ds(i * 512, 512)
            value = left * first[at, cols] + right * second[at, cols]
            first[at, cols] = value
            square = value * value
            out.append(acc[i] + square[:8] + square[8:])
        return tuple(out)

    acc = tuple(jnp.zeros((8, 512), jnp.float32) for _ in range(total // 512))
    for group, (low, size) in zip(loads, parts):
        for copy in group:
            copy.wait()
        acc = lax.fori_loop(low // ROWS, (low + size) // ROWS, mixed, acc)
    for i, value in enumerate(acc):
        sums[me, :, pl.ds(i * 512, 512)] = jnp.sum(value, axis=0, keepdims=True)

    pl.semaphore_wait(barrier, n - 1)

    def sum_copy(step, source):
        return pltpu.make_async_remote_copy(
            src_ref=sums.at[source], dst_ref=sums.at[source], send_sem=sum_send.at[step], recv_sem=sum_recv.at[source],
            device_id={"shard": lax.rem(me + step, n)}, device_id_type=MESH)

    for step in range(1, n):
        sum_copy(step, me).start()
    for step in range(1, n):
        sum_copy(step, lax.rem(me + step, n)).wait_recv()
    whole = sums[0]
    for source in range(1, n):
        whole = whole + sums[source]
    scale = jnp.sqrt(whole)
    scale_ref[...] = scale
    inverse = jnp.broadcast_to(1.0 / scale, (8, total))

    def copy(way, source, c):
        low, size = pieces[c]
        target = (jnp.minimum(z + 1, line - 1) * 2 + y, jnp.maximum(z - 1, 0) * 2 + y, other)[way]
        ref = buf.at[source, pl.ds(low, size), :]
        return pltpu.make_async_remote_copy(
            src_ref=ref, dst_ref=ref, send_sem=send_sem.at[way, source, c], recv_sem=recv_sem.at[source, c],
            device_id={"shard": target}, device_id_type=MESH)

    sent = []

    up, down = z < line - 1, z > 0

    def scaled(block, carry):
        at = pl.ds(pl.multiple_of(block * ROWS, ROWS), ROWS)
        for i in range(total // 512):
            cols = pl.ds(i * 512, 512)
            wide = jnp.concatenate([inverse[:, i * 512:(i + 1) * 512]] * 2, axis=0)
            buf[me, at, cols] = (first[at, cols] * wide).astype(buf.dtype)
        return carry

    def issue(condition, way, source, c):
        @pl.when(condition)
        def _():
            copy(way, source, c).start()
        sent.append((condition, way, source, c))

    always = z >= 0

    def issue_own(c):
        issue(up, 0, me, c)
        issue(down, 1, me, c)
        issue(always, 2, me, c)

    for c, (low, size) in enumerate(pieces):
        lax.fori_loop(low // ROWS, (low + size) // ROWS, scaled, 0)
        if c:
            issue_own(c - 1)
    issue_own(len(pieces) - 1)

    def pass_on(condition, source, c, ways):
        @pl.when(condition)
        def _():
            copy(2, source, c).wait_recv()
        for extra, way in ways:
            issue(condition & extra, way, source, c)

    def relay(step):
        for c in range(near, len(pieces)):
            if step == 0:
                pass_on(always, other, c, [(up, 0), (down, 1)])
            else:
                pass_on(z >= step, other - 2 * step, c, [(up, 0)])
                pass_on(z + step < line, other + 2 * step, c, [(down, 1)])

    for step in range(1, line):
        for c in range(len(pieces)):
            across = [(always, 2)] if c < near else []
            pass_on(z >= step, me - 2 * step, c, [(up, 0)] + across)
            pass_on(z + step < line, me + 2 * step, c, [(down, 1)] + across)
        relay(step - 1)
    relay(line - 1)
    for c in range(near):
        pass_on(always, other, c, [])
    for step in range(1, line):
        for c in range(near):
            pass_on(z >= step, other - 2 * step, c, [])
            pass_on(z + step < line, other + 2 * step, c, [])
    for condition, way, source, c in sent:
        @pl.when(condition)
        def _():
            copy(way, source, c).wait_send()
    for step in range(1, n):
        sum_copy(step, me).wait_send()


def store_kernel(n, widths, buf, scale_ref, *refs):
    outs, scales, sem = refs[:3], refs[3:6], refs[6]
    rows = buf.shape[1]
    copies = []
    for source in range(n):
        start = 0
        for i, width in enumerate(widths):
            copies.append(pltpu.make_async_copy(
                buf.at[source, :, pl.ds(start, width)], outs[i].at[pl.ds(source * rows, rows), :], sem.at[source, i]))
            copies[-1].start()
            start += width
    start = 0
    for i, width in enumerate(widths):
        scales[i][...] = scale_ref[:, start:start + width]
        start += width
    for copy in copies:
        copy.wait()


def routed(n, one_query, other_query, one_key, other_key, one_value, other_value, mix_share, norm_gain):
    widths = (one_query.shape[1], one_key.shape[1], one_value.shape[1])
    rows, total = one_query.shape[0], sum(widths)
    pieces = len(plan(rows, n // 2)[0])
    vmem = pl.BlockSpec(memory_space=pltpu.VMEM)
    hbm = pl.BlockSpec(memory_space=pl.ANY)
    buf, scale = pl.pallas_call(
        functools.partial(gather_kernel, n, widths),
        out_shape=(pltpu.VMEM((n, rows, total), jnp.bfloat16), pltpu.VMEM((1, total), jnp.float32)),
        in_specs=[vmem] * 2 + [hbm] * 6,
        out_specs=(vmem, vmem),
        scratch_shapes=[
            pltpu.VMEM((rows, total), jnp.float32),
            pltpu.VMEM((rows, total), jnp.float32),
            pltpu.VMEM((n, 1, total), jnp.float32),
            pltpu.SemaphoreType.DMA((4, 6)),
            pltpu.SemaphoreType.DMA((n,)),
            pltpu.SemaphoreType.DMA((n,)),
            pltpu.SemaphoreType.DMA((3, n, pieces)),
            pltpu.SemaphoreType.DMA((n, pieces)),
        ],
        compiler_params=pltpu.CompilerParams(collective_id=0, has_side_effects=True, vmem_limit_bytes=44 * 2**20),
    )(mix_share[:, None], norm_gain[:, None], one_query, other_query, one_key, other_key, one_value, other_value)
    outs = pl.pallas_call(
        functools.partial(store_kernel, n, widths),
        out_shape=tuple(jax.ShapeDtypeStruct((n * rows, width), jnp.bfloat16) for width in widths)
        + tuple(jax.ShapeDtypeStruct((1, width), jnp.float32) for width in widths),
        in_specs=[vmem, vmem],
        out_specs=(hbm,) * 3 + (vmem,) * 3,
        scratch_shapes=[pltpu.SemaphoreType.DMA((n, 3))],
        compiler_params=pltpu.CompilerParams(vmem_limit_bytes=2**20),
    )(pltpu.with_memory_space_constraint(buf, pltpu.VMEM), pltpu.with_memory_space_constraint(scale, pltpu.VMEM))
    return outs[:3] + tuple(out[0] for out in outs[3:])


def solution(mesh):
    n = mesh.shape["shard"]

    def body(*args):
        if n % 2 or n < 4 or args[0].shape[0] % ROWS or args[0].shape[0] < 6 * ROWS:
            return plain(*args)
        return routed(n, *args)

    return jax.shard_map(
        body,
        mesh=mesh,
        in_specs=(
            P("shard", "width"),
            P("shard", "width"),
            P("shard", "width"),
            P("shard", "width"),
            P("shard", "width"),
            P("shard", "width"),
            P("shard"),
            P("shard"),
        ),
        out_specs=(
            P(None, "width"),
            P(None, "width"),
            P(None, "width"),
            P("width"),
            P("width"),
            P("width"),
        ),
        check_vma=False,
    )
```

```python
import functools

import jax
import jax.numpy as jnp
from jax import lax
from jax.experimental import pallas as pl
from jax.experimental.pallas import tpu as pltpu
from jax.sharding import PartitionSpec as P

MESH = pl.DeviceIdType.MESH
ROWS = 16
TILE = 8
LANES = 128


def plain(one_query, other_query, one_key, other_key, one_value, other_value, mix_share, norm_gain):
    result_query = mix_share[:, None] * one_query + (1.0 - mix_share[:, None]) * other_query
    result_key = mix_share[:, None] * one_key + (1.0 - mix_share[:, None]) * other_key
    result_value = mix_share[:, None] * one_value + (1.0 - mix_share[:, None]) * other_value
    result_gained_query = result_query * norm_gain[:, None]
    result_gained_key = result_key * norm_gain[:, None]
    result_gained_value = result_value * norm_gain[:, None]
    total_query, total_key, total_value = lax.psum(
        (
            jnp.sum(result_gained_query * result_gained_query, axis=0),
            jnp.sum(result_gained_key * result_gained_key, axis=0),
            jnp.sum(result_gained_value * result_gained_value, axis=0),
        ),
        "shard",
    )
    scale_query = jnp.sqrt(total_query)
    scale_key = jnp.sqrt(total_key)
    scale_value = jnp.sqrt(total_value)
    narrow_query, narrow_key, narrow_value = (
        (result_gained_query / scale_query).astype(jnp.bfloat16),
        (result_gained_key / scale_key).astype(jnp.bfloat16),
        (result_gained_value / scale_value).astype(jnp.bfloat16),
    )
    final_query, final_key, final_value = (
        lax.all_gather(narrow_query, "shard", axis=0, tiled=True),
        lax.all_gather(narrow_key, "shard", axis=0, tiled=True),
        lax.all_gather(narrow_value, "shard", axis=0, tiled=True),
    )
    return (final_query, final_key, final_value, scale_query, scale_key, scale_value)


def cuts(start, end, parts, unit):
    edges = [start + (end - start) // unit * part // parts * unit for part in range(parts)] + [end]
    return [(low, high - low) for low, high in zip(edges, edges[1:])]


def plan(rows, line):
    far = max(1, round(rows / (2 * (line - 1) * TILE))) * TILE
    pieces = cuts(0, rows - far, 3, ROWS)
    return pieces + [(rows - far, far)], len(pieces)


def gather_kernel(n, widths, share_ref, gain_ref, *refs):
    ins, (buf, scale_ref, first, second, left, right, sums, in_sem, sum_send, sum_recv, send_sem, recv_sem) = refs[:6], refs[6:]
    rows = first.shape[0]
    total = sum(widths)
    line = n // 2
    me = lax.axis_index("shard")
    z, y = me // 2, me % 2
    other = z * 2 + 1 - y
    pieces, near = plan(rows, line)
    starts = [sum(widths[:i]) for i in range(len(widths))]

    loads = []
    parts = cuts(0, rows, 4, ROWS)
    for p, (low, size) in enumerate(parts):
        group = []
        for i, ref in enumerate(ins):
            dest = (first, second)[i % 2].at[pl.ds(low, size), pl.ds(starts[i // 2], widths[i // 2])]
            copy = pltpu.make_async_copy(ref.at[pl.ds(low, size), :], dest, in_sem.at[p, i])
            copy.start()
            group.append(copy)
        loads.append(group)

    barrier = pltpu.get_barrier_semaphore()
    for step in range(1, n):
        pl.semaphore_signal(barrier, inc=1, device_id={"shard": lax.rem(me + step, n)}, device_id_type=MESH)

    for low in range(0, rows, LANES):
        size = min(LANES, rows - low)
        share, gain = share_ref[:, low:low + size], gain_ref[:, low:low + size]
        for ref, row in ((left, share * gain), (right, (1.0 - share) * gain)):
            ref[pl.ds(low, size), :] = jnp.transpose(jnp.broadcast_to(row, (LANES, size)))

    def mixed(block, acc):
        at = pl.ds(pl.multiple_of(block * ROWS, ROWS), ROWS)
        ours, theirs = (jnp.concatenate([ref[at, :]] * 4, axis=1) for ref in (left, right))
        out = []
        for i in range(len(acc)):
            cols = pl.ds(i * 512, 512)
            value = ours * first[at, cols] + theirs * second[at, cols]
            first[at, cols] = value
            square = value * value
            out.append(acc[i] + square[:8] + square[8:])
        return tuple(out)

    acc = tuple(jnp.zeros((8, 512), jnp.float32) for _ in range(total // 512))
    for group, (low, size) in zip(loads, parts):
        for copy in group:
            copy.wait()
        acc = lax.fori_loop(low // ROWS, (low + size) // ROWS, mixed, acc)
    for i, value in enumerate(acc):
        sums[me, :, pl.ds(i * 512, 512)] = jnp.sum(value, axis=0, keepdims=True)

    pl.semaphore_wait(barrier, n - 1)

    def sum_copy(step, source):
        return pltpu.make_async_remote_copy(
            src_ref=sums.at[source], dst_ref=sums.at[source], send_sem=sum_send.at[step], recv_sem=sum_recv.at[source],
            device_id={"shard": lax.rem(me + step, n)}, device_id_type=MESH)

    for step in range(1, n):
        sum_copy(step, me).start()
    for step in range(1, n):
        sum_copy(step, lax.rem(me + step, n)).wait_recv()
    whole = sums[0]
    for source in range(1, n):
        whole = whole + sums[source]
    scale = jnp.sqrt(whole)
    scale_ref[...] = scale
    inverse = jnp.broadcast_to(1.0 / scale, (8, total))

    def copy(way, source, c):
        low, size = pieces[c]
        target = (jnp.minimum(z + 1, line - 1) * 2 + y, jnp.maximum(z - 1, 0) * 2 + y, other)[way]
        ref = buf.at[source, pl.ds(low, size), :]
        return pltpu.make_async_remote_copy(
            src_ref=ref, dst_ref=ref, send_sem=send_sem.at[way, source, c], recv_sem=recv_sem.at[source, c],
            device_id={"shard": target}, device_id_type=MESH)

    sent = []

    up, down = z < line - 1, z > 0

    def scaled(block, carry):
        at = pl.ds(pl.multiple_of(block * ROWS, ROWS), ROWS)
        for i in range(total // 512):
            cols = pl.ds(i * 512, 512)
            wide = jnp.concatenate([inverse[:, i * 512:(i + 1) * 512]] * 2, axis=0)
            buf[me, at, cols] = (first[at, cols] * wide).astype(buf.dtype)
        return carry

    def issue(condition, way, source, c):
        @pl.when(condition)
        def _():
            copy(way, source, c).start()
        sent.append((condition, way, source, c))

    always = z >= 0

    def issue_own(c):
        issue(up, 0, me, c)
        issue(down, 1, me, c)
        issue(always, 2, me, c)

    done = 0
    for c, (low, size) in enumerate(pieces):
        lax.fori_loop(done, pl.cdiv(low + size, ROWS), scaled, 0)
        done = pl.cdiv(low + size, ROWS)
        if c:
            issue_own(c - 1)
    issue_own(len(pieces) - 1)

    def pass_on(condition, source, c, ways):
        @pl.when(condition)
        def _():
            copy(2, source, c).wait_recv()
        for extra, way in ways:
            issue(condition & extra, way, source, c)

    def relay(step):
        for c in range(near, len(pieces)):
            if step == 0:
                pass_on(always, other, c, [(up, 0), (down, 1)])
            else:
                pass_on(z >= step, other - 2 * step, c, [(up, 0)])
                pass_on(z + step < line, other + 2 * step, c, [(down, 1)])

    for step in range(1, line):
        for c in range(len(pieces)):
            across = [(always, 2)] if c < near else []
            pass_on(z >= step, me - 2 * step, c, [(up, 0)] + across)
            pass_on(z + step < line, me + 2 * step, c, [(down, 1)] + across)
        relay(step - 1)
    relay(line - 1)
    for c in range(near):
        pass_on(always, other, c, [])
    for step in range(1, line):
        for c in range(near):
            pass_on(z >= step, other - 2 * step, c, [])
            pass_on(z + step < line, other + 2 * step, c, [])
    for condition, way, source, c in sent:
        @pl.when(condition)
        def _():
            copy(way, source, c).wait_send()
    for step in range(1, n):
        sum_copy(step, me).wait_send()


def store_kernel(n, widths, buf, scale_ref, *refs):
    outs, scales, sem = refs[:3], refs[3:6], refs[6]
    rows = buf.shape[1]
    copies = []
    for source in range(n):
        start = 0
        for i, width in enumerate(widths):
            copies.append(pltpu.make_async_copy(
                buf.at[source, :, pl.ds(start, width)], outs[i].at[pl.ds(source * rows, rows), :], sem.at[source, i]))
            copies[-1].start()
            start += width
    start = 0
    for i, width in enumerate(widths):
        scales[i][...] = scale_ref[:, start:start + width]
        start += width
    for copy in copies:
        copy.wait()


def routed(n, one_query, other_query, one_key, other_key, one_value, other_value, mix_share, norm_gain):
    widths = (one_query.shape[1], one_key.shape[1], one_value.shape[1])
    rows, total = one_query.shape[0], sum(widths)
    pieces = len(plan(rows, n // 2)[0])
    vmem = pl.BlockSpec(memory_space=pltpu.VMEM)
    hbm = pl.BlockSpec(memory_space=pl.ANY)
    buf, scale = pl.pallas_call(
        functools.partial(gather_kernel, n, widths),
        out_shape=(pltpu.VMEM((n, rows, total), jnp.bfloat16), pltpu.VMEM((1, total), jnp.float32)),
        in_specs=[vmem] * 2 + [hbm] * 6,
        out_specs=(vmem, vmem),
        scratch_shapes=[
            pltpu.VMEM((rows, total), jnp.float32),
            pltpu.VMEM((rows, total), jnp.float32),
            pltpu.VMEM((rows, LANES), jnp.float32),
            pltpu.VMEM((rows, LANES), jnp.float32),
            pltpu.VMEM((n, 1, total), jnp.float32),
            pltpu.SemaphoreType.DMA((4, 6)),
            pltpu.SemaphoreType.DMA((n,)),
            pltpu.SemaphoreType.DMA((n,)),
            pltpu.SemaphoreType.DMA((3, n, pieces)),
            pltpu.SemaphoreType.DMA((n, pieces)),
        ],
        compiler_params=pltpu.CompilerParams(collective_id=0, has_side_effects=True, vmem_limit_bytes=44 * 2**20),
    )(mix_share[None, :], norm_gain[None, :], one_query, other_query, one_key, other_key, one_value, other_value)
    outs = pl.pallas_call(
        functools.partial(store_kernel, n, widths),
        out_shape=tuple(jax.ShapeDtypeStruct((n * rows, width), jnp.bfloat16) for width in widths)
        + tuple(jax.ShapeDtypeStruct((1, width), jnp.float32) for width in widths),
        in_specs=[vmem, vmem],
        out_specs=(hbm,) * 3 + (vmem,) * 3,
        scratch_shapes=[pltpu.SemaphoreType.DMA((n, 3))],
        compiler_params=pltpu.CompilerParams(vmem_limit_bytes=2**20),
    )(pltpu.with_memory_space_constraint(buf, pltpu.VMEM), pltpu.with_memory_space_constraint(scale, pltpu.VMEM))
    return outs[:3] + tuple(out[0] for out in outs[3:])


def solution(mesh):
    n = mesh.shape["shard"]

    def body(*args):
        if n % 2 or n < 4 or args[0].shape[0] % ROWS or args[0].shape[0] < 6 * ROWS:
            return plain(*args)
        return routed(n, *args)

    return jax.shard_map(
        body,
        mesh=mesh,
        in_specs=(
            P("shard", "width"),
            P("shard", "width"),
            P("shard", "width"),
            P("shard", "width"),
            P("shard", "width"),
            P("shard", "width"),
            P("shard"),
            P("shard"),
        ),
        out_specs=(
            P(None, "width"),
            P(None, "width"),
            P(None, "width"),
            P("width"),
            P("width"),
            P("width"),
        ),
        check_vma=False,
    )
```

```python
import functools

import jax
import jax.numpy as jnp
from jax import lax
from jax.experimental import pallas as pl
from jax.experimental.pallas import tpu as pltpu
from jax.sharding import PartitionSpec as P

MESH = pl.DeviceIdType.MESH
ROWS = 16
TILE = 8
LANES = 128
EARLY = ROWS


def plain(one_query, other_query, one_key, other_key, one_value, other_value, mix_share, norm_gain):
    result_query = mix_share[:, None] * one_query + (1.0 - mix_share[:, None]) * other_query
    result_key = mix_share[:, None] * one_key + (1.0 - mix_share[:, None]) * other_key
    result_value = mix_share[:, None] * one_value + (1.0 - mix_share[:, None]) * other_value
    result_gained_query = result_query * norm_gain[:, None]
    result_gained_key = result_key * norm_gain[:, None]
    result_gained_value = result_value * norm_gain[:, None]
    total_query, total_key, total_value = lax.psum(
        (
            jnp.sum(result_gained_query * result_gained_query, axis=0),
            jnp.sum(result_gained_key * result_gained_key, axis=0),
            jnp.sum(result_gained_value * result_gained_value, axis=0),
        ),
        "shard",
    )
    scale_query = jnp.sqrt(total_query)
    scale_key = jnp.sqrt(total_key)
    scale_value = jnp.sqrt(total_value)
    narrow_query, narrow_key, narrow_value = (
        (result_gained_query / scale_query).astype(jnp.bfloat16),
        (result_gained_key / scale_key).astype(jnp.bfloat16),
        (result_gained_value / scale_value).astype(jnp.bfloat16),
    )
    final_query, final_key, final_value = (
        lax.all_gather(narrow_query, "shard", axis=0, tiled=True),
        lax.all_gather(narrow_key, "shard", axis=0, tiled=True),
        lax.all_gather(narrow_value, "shard", axis=0, tiled=True),
    )
    return (final_query, final_key, final_value, scale_query, scale_key, scale_value)


def cuts(start, end, parts, unit):
    edges = [start + (end - start) // unit * part // parts * unit for part in range(parts)] + [end]
    return [(low, high - low) for low, high in zip(edges, edges[1:])]


def plan(rows, line):
    far = max(1, round(rows / (2 * (line - 1) * TILE))) * TILE
    pieces = [(0, EARLY)] + cuts(EARLY, rows - far, 2, ROWS)
    return pieces + [(rows - far, far)], len(pieces)


def gather_kernel(n, widths, share_ref, gain_ref, *refs):
    ins, (buf, scale_ref, first, second, left, right, sums, early, in_sem, sum_send, sum_recv, early_send, early_recv, send_sem, recv_sem) = refs[:6], refs[6:]
    rows = first.shape[0]
    total = sum(widths)
    line = n // 2
    me = lax.axis_index("shard")
    z, y = me // 2, me % 2
    other = z * 2 + 1 - y
    pieces, near = plan(rows, line)
    starts = [sum(widths[:i]) for i in range(len(widths))]

    loads = []
    parts = cuts(0, rows, 4, ROWS)
    for p, (low, size) in enumerate(parts):
        group = []
        for i, ref in enumerate(ins):
            dest = (first, second)[i % 2].at[pl.ds(low, size), pl.ds(starts[i // 2], widths[i // 2])]
            copy = pltpu.make_async_copy(ref.at[pl.ds(low, size), :], dest, in_sem.at[p, i])
            copy.start()
            group.append(copy)
        loads.append(group)

    barrier = pltpu.get_barrier_semaphore()
    for step in range(1, n):
        pl.semaphore_signal(barrier, inc=1, device_id={"shard": lax.rem(me + step, n)}, device_id_type=MESH)

    for low in range(0, rows, LANES):
        size = min(LANES, rows - low)
        share, gain = share_ref[:, low:low + size], gain_ref[:, low:low + size]
        for ref, row in ((left, share * gain), (right, (1.0 - share) * gain)):
            ref[pl.ds(low, size), :] = jnp.transpose(jnp.broadcast_to(row, (LANES, size)))

    def mixed(block, acc):
        at = pl.ds(pl.multiple_of(block * ROWS, ROWS), ROWS)
        ours, theirs = (jnp.concatenate([ref[at, :]] * 4, axis=1) for ref in (left, right))
        out = []
        for i in range(len(acc)):
            cols = pl.ds(i * 512, 512)
            value = ours * first[at, cols] + theirs * second[at, cols]
            first[at, cols] = value
            square = value * value
            out.append(acc[i] + square[:8] + square[8:])
        return tuple(out)

    acc = tuple(jnp.zeros((8, 512), jnp.float32) for _ in range(total // 512))
    for group, (low, size) in zip(loads, parts):
        for copy in group:
            copy.wait()
        acc = lax.fori_loop(low // ROWS, (low + size) // ROWS, mixed, acc)
    for i, value in enumerate(acc):
        sums[me, :, pl.ds(i * 512, 512)] = jnp.sum(value, axis=0, keepdims=True)

    pl.semaphore_wait(barrier, n - 1)

    def sum_copy(target, source):
        return pltpu.make_async_remote_copy(
            src_ref=sums.at[source], dst_ref=sums.at[source], send_sem=sum_send.at[target], recv_sem=sum_recv.at[source],
            device_id={"shard": target}, device_id_type=MESH)

    peers = [jnp.where(z < line // 2, line - 1 - k, k) * 2 + side for k in range(line) for side in (1 - y, y)]
    for peer in peers:
        @pl.when(peer != me)
        def _():
            sum_copy(peer, me).start()

    up, down, always = z < line - 1, z > 0, z >= 0
    targets = (jnp.minimum(z + 1, line - 1) * 2 + y, jnp.maximum(z - 1, 0) * 2 + y, other)

    def early_copy(way):
        return pltpu.make_async_remote_copy(
            src_ref=first.at[pl.ds(0, EARLY), :], dst_ref=early.at[way], send_sem=early_send.at[way],
            recv_sem=early_recv.at[way], device_id={"shard": targets[way]}, device_id_type=MESH)

    for way, condition in enumerate((up, down, always)):
        @pl.when(condition)
        def _():
            early_copy(way).start()

    for peer in peers:
        @pl.when(peer != me)
        def _():
            sum_copy(other, peer).wait_recv()
    whole = sums[0]
    for source in range(1, n):
        whole = whole + sums[source]
    scale = jnp.sqrt(whole)
    scale_ref[...] = scale
    inverse = jnp.broadcast_to(1.0 / scale, (8, total))

    def copy(way, source, c):
        low, size = pieces[c]
        ref = buf.at[source, pl.ds(low, size), :]
        return pltpu.make_async_remote_copy(
            src_ref=ref, dst_ref=ref, send_sem=send_sem.at[way, source, c], recv_sem=recv_sem.at[source, c],
            device_id={"shard": targets[way]}, device_id_type=MESH)

    sent = []

    def scaled(source, ref):
        def step(block, carry):
            at = pl.ds(pl.multiple_of(block * ROWS, ROWS), ROWS)
            for i in range(total // 512):
                cols = pl.ds(i * 512, 512)
                wide = jnp.concatenate([inverse[:, i * 512:(i + 1) * 512]] * 2, axis=0)
                buf[source, at, cols] = (ref[at, cols] * wide).astype(buf.dtype)
            return carry
        return step

    def issue(condition, way, source, c):
        @pl.when(condition)
        def _():
            copy(way, source, c).start()
        sent.append((condition, way, source, c))

    def issue_own(c):
        issue(up, 0, me, c)
        issue(down, 1, me, c)
        issue(always, 2, me, c)

    done = 0
    for c, (low, size) in enumerate(pieces):
        lax.fori_loop(done, pl.cdiv(low + size, ROWS), scaled(me, first), 0)
        done = pl.cdiv(low + size, ROWS)
        if c > 1:
            issue_own(c - 1)
    issue_own(len(pieces) - 1)

    for way, (condition, source) in enumerate(((down, me - 2), (up, me + 2), (always, other))):
        @pl.when(condition)
        def _():
            early_copy(way).wait_recv()
            lax.fori_loop(0, EARLY // ROWS, scaled(source, early.at[way]), 0)
    issue(down & up, 0, me - 2, 0)
    issue(down, 2, me - 2, 0)
    issue(up & down, 1, me + 2, 0)
    issue(up, 2, me + 2, 0)

    def pass_on(condition, source, c, ways):
        @pl.when(condition)
        def _():
            copy(2, source, c).wait_recv()
        for extra, way in ways:
            issue(condition & extra, way, source, c)

    def relay(step):
        for c in range(near, len(pieces)):
            if step == 0:
                pass_on(always, other, c, [(up, 0), (down, 1)])
            else:
                pass_on(z >= step, other - 2 * step, c, [(up, 0)])
                pass_on(z + step < line, other + 2 * step, c, [(down, 1)])

    for step in range(1, line):
        for c in range(1 if step == 1 else 0, len(pieces)):
            across = [(always, 2)] if c < near else []
            pass_on(z >= step, me - 2 * step, c, [(up, 0)] + across)
            pass_on(z + step < line, me + 2 * step, c, [(down, 1)] + across)
        relay(step - 1)
    relay(line - 1)
    for c in range(1, near):
        pass_on(always, other, c, [])
    for step in range(1, line):
        for c in range(near):
            pass_on(z >= step, other - 2 * step, c, [])
            pass_on(z + step < line, other + 2 * step, c, [])
    for condition, way, source, c in sent:
        @pl.when(condition)
        def _():
            copy(way, source, c).wait_send()
    for way, condition in enumerate((up, down, always)):
        @pl.when(condition)
        def _():
            early_copy(way).wait_send()
    for peer in peers:
        @pl.when(peer != me)
        def _():
            sum_copy(peer, me).wait_send()


def store_kernel(n, widths, buf, scale_ref, *refs):
    outs, scales, sem = refs[:3], refs[3:6], refs[6]
    rows = buf.shape[1]
    copies = []
    for source in range(n):
        start = 0
        for i, width in enumerate(widths):
            copies.append(pltpu.make_async_copy(
                buf.at[source, :, pl.ds(start, width)], outs[i].at[pl.ds(source * rows, rows), :], sem.at[source, i]))
            copies[-1].start()
            start += width
    start = 0
    for i, width in enumerate(widths):
        scales[i][...] = scale_ref[:, start:start + width]
        start += width
    for copy in copies:
        copy.wait()


def routed(n, one_query, other_query, one_key, other_key, one_value, other_value, mix_share, norm_gain):
    widths = (one_query.shape[1], one_key.shape[1], one_value.shape[1])
    rows, total = one_query.shape[0], sum(widths)
    pieces = len(plan(rows, n // 2)[0])
    vmem = pl.BlockSpec(memory_space=pltpu.VMEM)
    hbm = pl.BlockSpec(memory_space=pl.ANY)
    buf, scale = pl.pallas_call(
        functools.partial(gather_kernel, n, widths),
        out_shape=(pltpu.VMEM((n, rows, total), jnp.bfloat16), pltpu.VMEM((1, total), jnp.float32)),
        in_specs=[vmem] * 2 + [hbm] * 6,
        out_specs=(vmem, vmem),
        scratch_shapes=[
            pltpu.VMEM((rows, total), jnp.float32),
            pltpu.VMEM((rows, total), jnp.float32),
            pltpu.VMEM((rows, LANES), jnp.float32),
            pltpu.VMEM((rows, LANES), jnp.float32),
            pltpu.VMEM((n, 1, total), jnp.float32),
            pltpu.VMEM((3, EARLY, total), jnp.float32),
            pltpu.SemaphoreType.DMA((4, 6)),
            pltpu.SemaphoreType.DMA((n,)),
            pltpu.SemaphoreType.DMA((n,)),
            pltpu.SemaphoreType.DMA((3,)),
            pltpu.SemaphoreType.DMA((3,)),
            pltpu.SemaphoreType.DMA((3, n, pieces)),
            pltpu.SemaphoreType.DMA((n, pieces)),
        ],
        compiler_params=pltpu.CompilerParams(collective_id=0, has_side_effects=True, vmem_limit_bytes=44 * 2**20),
    )(mix_share[None, :], norm_gain[None, :], one_query, other_query, one_key, other_key, one_value, other_value)
    outs = pl.pallas_call(
        functools.partial(store_kernel, n, widths),
        out_shape=tuple(jax.ShapeDtypeStruct((n * rows, width), jnp.bfloat16) for width in widths)
        + tuple(jax.ShapeDtypeStruct((1, width), jnp.float32) for width in widths),
        in_specs=[vmem, vmem],
        out_specs=(hbm,) * 3 + (vmem,) * 3,
        scratch_shapes=[pltpu.SemaphoreType.DMA((n, 3))],
        compiler_params=pltpu.CompilerParams(vmem_limit_bytes=2**20),
    )(pltpu.with_memory_space_constraint(buf, pltpu.VMEM), pltpu.with_memory_space_constraint(scale, pltpu.VMEM))
    return outs[:3] + tuple(out[0] for out in outs[3:])


def solution(mesh):
    n = mesh.shape["shard"]

    def body(*args):
        if n % 2 or n < 4 or args[0].shape[0] % ROWS or args[0].shape[0] < 6 * ROWS:
            return plain(*args)
        return routed(n, *args)

    return jax.shard_map(
        body,
        mesh=mesh,
        in_specs=(
            P("shard", "width"),
            P("shard", "width"),
            P("shard", "width"),
            P("shard", "width"),
            P("shard", "width"),
            P("shard", "width"),
            P("shard"),
            P("shard"),
        ),
        out_specs=(
            P(None, "width"),
            P(None, "width"),
            P(None, "width"),
            P("width"),
            P("width"),
            P("width"),
        ),
        check_vma=False,
    )
```
